32 devices in a mesh: groups: 2 (over y), ep: 4 (over z), tp: 2 (over x), dp: 2 (over core).
Axes of the slice: x: 2, y: 2, z: 4, core: 2. Of those that a mesh axis runs over, the one named last changes fastest.
Arguments:
- tokens: bfloat16 [256, 5120], P(('groups', 'ep', 'tp', 'dp')), parts along dimension 0, may hold values from -6 to 6
- route_weights: float32 [256, 8], P(('groups', 'ep', 'tp', 'dp')), parts along dimension 0, may hold values from 0.1 to 1
- expert_ids: int32 [256, 8], P(('groups', 'ep', 'tp', 'dp')), parts along dimension 0, may hold values from 0 to 31, all different within a row; in each aligned block of 8 rows (0 to 7, 8 to 15, ...) at most 4 rows name the same one
- gate_weight: bfloat16 [32, 5120, 1024], P('ep', None, ('tp', 'dp')), may hold values from -0.078125 to 0.078125
- up_weight: bfloat16 [32, 5120, 1024], P('ep', None, ('tp', 'dp')), may hold values from -0.078125 to 0.078125
- down_weight: bfloat16 [32, 1024, 5120], P('ep', None, ('tp', 'dp')), may hold values from -0.1875 to 0.1875
Outputs:
- combined: bfloat16 [256, 5120], P(('groups', 'ep', 'tp', 'dp')), parts along dimension 0
The draws below stay inside these ranges and needn't reach their ends.
There are 2 independent parts, one for each index of `groups`. The reference program is written for one: setup_inputs(seed, part) draws one part's arguments, and reference() takes and returns one part's arrays. A program takes and returns all parts, laid end to end along the dimension named above; an argument that names none is the same for every part. Nothing has to cross between parts.
Inputs may be any that keep to these rules, and one draw needn't show every extreme that they name: `expert_ids`: each row names 8 different experts. Among the 8 rows of one device no expert is named more than 4 times, and in every draw some device's rows name some expert exactly 4 times.
All inputs are finite; a program needn't handle non-finite values.
Results may differ from the reference program's by a relative error of at most 0.0057.
Values may be sent and summed in bfloat16 or wider, within the bound.
No kernel may reach another device: no remote copies, remote signals or barrier semaphores. Data moves between devices by JAX's collectives and lax.ppermute only.
A program may use at most 128 MiB of HBM per device.

```python
import math
import jax
import jax.numpy as jnp
import numpy as np
from jax import lax

D = 5120
FF = 1024
EXPERTS = 32
TOP = 8
TOK_DEV = 8
CAP = 4
TOKENS = 128
N_EP = 4
N_TP = 2
N_DP = 2


def block_levels(own_key, dims, shards, low, top_value):
    gain = 1.0
    for dim, shards_of in shards:
        heights = jax.random.uniform(jax.random.fold_in(jax.random.fold_in(own_key, 6), dim), (shards_of,), jnp.float32, low / len(shards), top_value / len(shards))
        gain = gain * jnp.repeat(jnp.exp(heights), dims[dim] // shards_of).reshape((-1,) + (1,) * (len(dims) - 1 - dim))
    return gain


def deal_out(key, own, number, rows, count, top, most, lean):
    sequence = jax.random.permutation(key, count)
    heavy_load, usual = portions_of(count, rows * top, most, lean, True), portions_of(count, rows * top, most, lean, False)
    places = jnp.arange(count)

    def named(tallies, turn):
        used = int((tallies > 0).sum())
        fixed = max(1, used // 4)
        passed = fixed + (places - fixed + turn * (used - fixed)) % max(1, count - fixed)
        return jnp.zeros((count,), jnp.int32).at[sequence[jnp.where(places < fixed, places, passed)]].set(jnp.asarray(tallies, jnp.int32))

    tallies = jnp.where(number % 4 == 0, named(heavy_load, number // 4), named(usual, number - number // 4 - 1))
    mixed = jax.random.permutation(jax.random.fold_in(own, 3), count)
    donor, sink = mixed[0:count // 2 * 2:2], mixed[1:count // 2 * 2:2]
    slack = jnp.minimum(tallies[donor] - 1, most - tallies[sink]) // 2
    slack = jnp.where((donor == sequence[0]) | (sink == sequence[0]) | (tallies[sink] == 0), 0, jnp.maximum(slack, 0))
    passed = jax.random.randint(jax.random.fold_in(own, 4), (count // 2,), 0, 1 << 20) % (slack + 1)
    tallies = tallies.at[donor].add(-passed).at[sink].add(passed)
    members = jnp.searchsorted(jnp.cumsum(tallies), jnp.arange(rows * top), side="right").astype(jnp.int32)
    grid = members.reshape(top, rows).T
    grid = grid[jax.random.permutation(jax.random.fold_in(own, 1), rows)]
    turn = jax.random.randint(jax.random.fold_in(own, 2), (rows, 1), 0, top)
    return jnp.take_along_axis(grid, (jnp.arange(top)[None, :] + turn) % top, axis=1)


def portions_of(number_of, total, most, lean, full):
    weights = [(1 << 20) // math.isqrt(rank ** lean) + 1 for rank in range(1, number_of + 1)]
    largest = most if full else min(most, max(-(-total // number_of), total * weights[0] // sum(weights)))
    least = 1 if total - largest >= number_of - 1 else 0
    given, spare = [largest] + [least] * (number_of - 1), total - largest - least * (number_of - 1)
    while spare > 0:
        candidates = [i for i in range(1, number_of) if given[i] < largest] or [i for i in range(1, number_of) if given[i] < most]
        mass, budget = sum([weights[i] for i in candidates]), spare
        for i in candidates:
            extra = min(most - given[i], max(1, budget * weights[i] // mass), spare)
            given[i] = given[i] + extra
            spare = spare - extra
    return np.array(given)


def normal_values(stream_key, dims, deviation, limit, shards=(), held_as=jnp.bfloat16):
    array = jax.random.normal(stream_key, dims, jnp.float32) * deviation
    if len(shards) > 0:
        array = block_levels(stream_key, dims, shards, -0.22, 0.18) * array
    return jnp.clip(array, min=-limit, max=limit).astype(held_as)


def setup_inputs(seed: int = 0, part: int = 0) -> dict:
    streams_of = jax.random.split(jax.random.key(seed), 7)
    own_keys = jax.random.split(jax.random.fold_in(streams_of[6], part), 7)
    tokens = normal_values(own_keys[0], (TOKENS, D), 1.0, 6.0, ((0, 16),))
    route_weights = jnp.clip(jnp.exp(math.log(1.0) - 2.3025851 * jax.random.uniform(own_keys[1], (TOKENS, TOP), jnp.float32) ** block_levels(own_keys[1], (TOKENS, TOP), ((0, 16),), -0.2, 0.2)), 0.1, 1.0)
    expert_ids_keys = jax.random.split(jax.random.fold_in(own_keys[2], 1), TOKENS // TOK_DEV)
    expert_ids_turns = jax.random.permutation(jax.random.fold_in(own_keys[2], 3), TOKENS // TOK_DEV)
    expert_ids = jax.vmap(lambda own, number: deal_out(jax.random.fold_in(own_keys[2], 2), own, number, TOK_DEV, EXPERTS, TOP, CAP, 2))(expert_ids_keys, expert_ids_turns).reshape((TOKENS, TOP))
    gate_weight = normal_values(streams_of[3], (EXPERTS, D, FF), D ** -0.5, 0.078125, ((0, 4), (2, 4)))
    up_weight = normal_values(streams_of[4], (EXPERTS, D, FF), D ** -0.5, 0.078125, ((0, 4), (2, 4)))
    down_weight = normal_values(streams_of[5], (EXPERTS, FF, D), FF ** -0.5, 0.1875, ((0, 4), (2, 4)))
    return dict(tokens=tokens, route_weights=route_weights, expert_ids=expert_ids, gate_weight=gate_weight, up_weight=up_weight, down_weight=down_weight)


def reference(tokens, route_weights, expert_ids, gate_weight, up_weight, down_weight):
    devices = N_EP * N_TP * N_DP
    blocks = expert_ids.reshape(devices, TOK_DEV * TOP)
    onehot = (blocks[:, :, None] == jnp.arange(EXPERTS, dtype=jnp.int32)[None, None, :]).astype(jnp.int32)
    slots = jnp.sum(onehot * jnp.cumsum(onehot, axis=1), axis=2) - 1
    device_ids = jnp.arange(devices, dtype=jnp.int32)[:, None]
    position = (device_ids * CAP + slots).reshape(-1).astype(jnp.int32)
    flat_ids = expert_ids.reshape(-1).astype(jnp.int32)
    owner = (jnp.arange(TOKENS * TOP, dtype=jnp.int32) // TOP).astype(jnp.int32)
    span = devices * CAP

    def one_expert(expert):
        index = jnp.where(flat_ids == expert, position, span).astype(jnp.int32)
        table = jnp.full((span,), TOKENS, jnp.int32).at[index].set(owner, mode="drop")
        rows = jnp.take(tokens, table, axis=0, mode="fill", fill_value=0)
        gate = jnp.dot(rows, gate_weight[expert], preferred_element_type=jnp.float32)
        up = jnp.dot(rows, up_weight[expert], preferred_element_type=jnp.float32)
        hidden = (jax.nn.silu(gate) * up).astype(jnp.bfloat16)
        return jnp.dot(hidden, down_weight[expert], preferred_element_type=jnp.float32).astype(jnp.bfloat16)

    outputs = lax.map(one_expert, jnp.arange(EXPERTS, dtype=jnp.int32))
    flat_out = outputs.reshape(EXPERTS * span, D)
    picked_index = (flat_ids * span + position).reshape(TOKENS, TOP).astype(jnp.int32)
    total = jnp.zeros((TOKENS, D), jnp.float32)
    for route in range(TOP):
        chosen = jnp.take(flat_out, picked_index[:, route], axis=0).astype(jnp.float32)
        total = total + route_weights[:, route:route + 1] * chosen
    return total.astype(jnp.bfloat16)
```

```python
import functools

import jax
import jax.numpy as jnp
from jax import lax
from jax.experimental import pallas as pl
from jax.experimental.pallas import tpu as pltpu
from jax.sharding import PartitionSpec as P


CAP = 4
LANES = 128
FEW = 4
ROWS = 128
F32, BF16 = jnp.float32, jnp.bfloat16
VMEM = pl.BlockSpec(memory_space=pltpu.VMEM)
HBM = pl.BlockSpec(memory_space=pltpu.HBM)
ANY = pl.BlockSpec(memory_space=pl.ANY)


def hbm(x):
    return pltpu.with_memory_space_constraint(x, pltpu.HBM)


def vmem(x):
    return pltpu.with_memory_space_constraint(x, pltpu.VMEM)


def mate(i, step, n):
    return i ^ step if n & (n - 1) == 0 else (step - i) % n


def mate_of(axis, step):
    n = lax.axis_size(axis)
    i = lax.axis_index(axis)
    return i ^ step if n & (n - 1) == 0 else lax.rem(step - i + n, n)


def places(n_tp, n_dp):
    t = [mate_of("tp", a) if a else lax.axis_index("tp") for a in range(n_tp)]
    d = [mate_of("dp", b) if b else lax.axis_index("dp") for b in range(n_dp)]
    return [t[a] * n_dp + d[b] for a in range(n_tp) for b in range(n_dp)]


def owners(n_ep):
    return [mate_of("ep", s) if s else lax.axis_index("ep") for s in range(n_ep)]


def meet(x, axis, step):
    n = lax.axis_size(axis)
    return lax.ppermute(x, axis, [(i, mate(i, step, n)) for i in range(n)])


def steps_of(n):
    return list(range(n - 1, 0, -1))


def call(kernel, in_specs, outs, args, scratch=(), limit=16, flops=0):
    return pl.pallas_call(
        kernel,
        in_specs=in_specs,
        out_specs=[VMEM] * len(outs),
        out_shape=[pltpu.VMEM(s, d) for s, d in outs],
        scratch_shapes=list(scratch),
        cost_estimate=pl.CostEstimate(
            flops=flops, bytes_accessed=flops // 64, transcendentals=0
        )
        if flops
        else None,
        compiler_params=pltpu.CompilerParams(vmem_limit_bytes=limit << 20),
    )(*args)


def pack_kernel(tok_hbm, weight_hbm, id_hbm, out_ref, weight_ref, id_ref, sems):
    tok, width = tok_hbm.shape
    top = id_hbm.shape[1]
    copies = [
        pltpu.make_async_copy(weight_hbm, weight_ref, sems.at[0]),
        pltpu.make_async_copy(id_hbm, id_ref, sems.at[1]),
        pltpu.make_async_copy(tok_hbm, out_ref.at[:, pl.ds(0, width)], sems.at[2]),
    ]
    for c in copies:
        c.start()
    for c in copies[:2]:
        c.wait()
    w = weight_ref[...]
    high = w.astype(BF16).astype(F32)
    pad = jnp.zeros((tok, LANES - 3 * top), F32)
    meta = jnp.concatenate([id_ref[...].astype(F32), high, w - high, pad], axis=1)
    out_ref[:, pl.ds(width, LANES)] = meta.astype(BF16)
    copies[2].wait()


def join_kernel(*refs):
    out_ref, rows = refs[-1], refs[0].shape[0]
    for i, ref in enumerate(refs[:-1]):
        out_ref[pl.ds(i * rows, rows), :] = ref[...]


def fetch_kernel(start, *refs):
    count = len(refs) - 3
    srcs, dst_ref, sems = refs[:count], refs[-2], refs[-1]
    copies = [
        pltpu.make_async_copy(srcs[k].at[start + i], dst_ref.at[k, i], sems.at[k, i])
        for i in range(dst_ref.shape[1])
        for k in range(count)
    ]
    for c in copies:
        c.start()
    for c in copies:
        c.wait()


def fetch(weights, start, count, after):
    return call(
        functools.partial(fetch_kernel, start),
        [HBM] * len(weights) + [VMEM],
        [((len(weights), count) + weights[0].shape[1:], weights[0].dtype)],
        [*map(hbm, weights), vmem(after)],
        [pltpu.SemaphoreType.DMA((len(weights), count))],
        limit=1,
        flops=int(6e8),
    )[0]


def prepare(x_ref, wt_ref, slot_ref, slot_t_ref, tok_refs, chunks, n_tp, n_dp, top, tok):
    pieces = n_tp * n_dp
    place = places(n_tp, n_dp)
    for c, owner in enumerate(chunks):
        for i in range(pieces):
            ref = tok_refs[c * pieces + i]
            if isinstance(owner, int):
                def put(e, carry, ref=ref, i=i):
                    to = pl.multiple_of((e * pieces + place[i]) * tok, tok)
                    x_ref[pl.ds(to, tok), :] = ref[pl.ds(pl.multiple_of(e * tok, tok), tok), :]
                    return carry

                lax.fori_loop(0, owner, put, 0)
                continue
            for k, s in enumerate(owner):
                e = mate_of("ep", s) if s else lax.axis_index("ep")
                to = pl.multiple_of((e * pieces + place[i]) * tok, tok)
                x_ref[pl.ds(to, tok), :] = ref[pl.ds(k * tok, tok), :]
    total = x_ref.shape[0]
    meta = x_ref[:, pl.ds(x_ref.shape[1] - LANES, LANES)].astype(F32)
    lane = lax.broadcasted_iota(jnp.int32, (total, LANES), 1).astype(F32)
    row = lax.broadcasted_iota(jnp.int32, (total, LANES), 0)
    named = jnp.zeros((total, LANES), F32)
    weight = jnp.zeros((total, LANES), F32)
    for k in range(top):
        hit = meta[:, k : k + 1] == lane
        value = meta[:, top + k : top + k + 1] + meta[:, 2 * top + k : 2 * top + k + 1]
        named = jnp.where(hit, 1.0, named)
        weight = jnp.where(hit, value, weight)
    rank = named
    back = 1
    while back < tok:
        moved = pltpu.roll(rank, back, axis=0)
        rank = rank + jnp.where(lax.rem(row, tok) >= back, moved, 0.0)
        back *= 2
    base = lax.div(row, tok).astype(F32) * float(CAP)
    slot = jnp.where(named > 0.0, base + rank - 1.0, -1.0)
    wt_ref[...] = weight
    slot_ref[...] = slot
    tall = min(total, ROWS)
    for b in range(total // tall):
        slot_t_ref[b] = slot[b * tall : (b + 1) * tall, :].T


def hidden_experts(experts, count, tok, x_ref, wt_ref, slot_t_ref, out_ref, source):
    total, width = x_ref.shape[0], x_ref.shape[1] - LANES
    tall = min(total, ROWS)
    for n, e in enumerate(experts):
        expert = lax.axis_index("ep") * count + e
        gate_ref, up_ref = source(e)

        def block(b, carry, n=n, expert=expert, gate_ref=gate_ref, up_ref=up_ref):
            r = b * tall if isinstance(b, int) else pl.multiple_of(b * tall, tall)
            rows = pl.ds(r, tall)
            line = slot_t_ref[b, pl.ds(expert, 1), :]
            x = x_ref[rows, pl.ds(0, width)]
            gate = jnp.dot(x, gate_ref[...], preferred_element_type=F32)
            up = jnp.dot(x, up_ref[...], preferred_element_type=F32)
            at = lax.broadcasted_iota(jnp.int32, (tall, LANES), 1) == expert
            scale = jnp.sum(jnp.where(at, wt_ref[rows, :], 0.0), axis=1, keepdims=True)
            hidden = (gate * (1.0 / (1.0 + jnp.exp(-gate))) * up * scale).astype(BF16)
            many = tall // tok * CAP
            first = b * many if isinstance(b, int) else pl.multiple_of(b * many, many)
            slot = lax.broadcasted_iota(jnp.int32, (many, tall), 0) + first
            pick = (slot.astype(F32) == line).astype(BF16)
            out_ref[n, pl.ds(first, many), :] = jnp.dot(
                pick, hidden, preferred_element_type=F32
            ).astype(BF16)
            return carry

        if total == tall:
            block(0, 0)
        else:
            lax.fori_loop(0, total // tall, block, 0)


def stream(srcs, dst_ref, sems, items):
    copies = {
        e: [
            pltpu.make_async_copy(src.at[e], dst_ref.at[k, i], sems.at[k, i])
            for k, src in enumerate(srcs)
        ]
        for i, e in enumerate(items)
    }
    for e in items:
        for c in copies[e]:
            c.start()
    return copies


def take_from(held, ready_ref, streamed, late_ref, copies):
    def source(e):
        if e in held:
            i, ref = held.index(e), ready_ref
        else:
            i, ref = streamed.index(e), late_ref
            for c in copies[e]:
                c.wait()
        return ref.at[0, i], ref.at[1, i]

    return source


def first_kernel(geometry, chunks, held, streamed, *refs):
    n_tp, n_dp, top, tok = geometry
    refs = list(refs)
    take = lambda n: [refs.pop(0) for _ in range(n)]
    tok_refs = take(len(chunks) * n_tp * n_dp)
    ready_ref = take(1)[0] if held else None
    weights = take(2)
    out_ref, slot_ref, x_ref, wt_ref, slot_t_ref, late_ref, sems = refs
    copies = stream(weights, late_ref, sems, streamed)
    prepare(x_ref, wt_ref, slot_ref, slot_t_ref, tok_refs, chunks, n_tp, n_dp, top, tok)
    source = take_from(held, ready_ref, streamed, late_ref, copies)
    count = weights[0].shape[0]
    hidden_experts(held + streamed, count, tok, x_ref, wt_ref, slot_t_ref, out_ref, source)


def second_kernel(tok, held, streamed, ready_ref, x_ref, wt_ref, slot_t_ref, *refs):
    gate_ref, up_ref, out_ref, late_ref, sems = refs
    copies = stream((gate_ref, up_ref), late_ref, sems, streamed)
    source = take_from(held, ready_ref, streamed, late_ref, copies)
    count = gate_ref.shape[0]
    hidden_experts(held + streamed, count, tok, x_ref, wt_ref, slot_t_ref, out_ref, source)


def down_kernel(n_ep, n_tp, n_dp, few, held, streamed, ahead, *refs):
    pieces = n_tp * n_dp
    refs = list(refs)
    take = lambda n: [refs.pop(0) for _ in range(n)]
    hid_refs = take(pieces)
    slot_ref, down_ref = take(2)
    now_ref, before_ref = take(2) if held else (None, None)
    late_ref, sems, all_ref = refs[-3:]
    if ahead:
        acc_ref, next_ref = take(2)
        next_sems = refs[-4]
    else:
        outs, acc_ref = refs[:-4], refs[-4]
    copies = stream((down_ref,), late_ref, sems, streamed)
    if ahead:
        more = stream((down_ref,), next_ref, next_sems, ahead)
    count = down_ref.shape[0]
    total = slot_ref.shape[0]
    _, slots, part = hid_refs[0].shape
    full = part * pieces
    ep_me = lax.axis_index("ep")
    place = places(n_tp, n_dp)
    owner = owners(n_ep) if few else []
    tall = min(total, ROWS)
    many = slots * tall // total
    experts = held + streamed
    for n, e in enumerate(experts):
        at = lax.broadcasted_iota(jnp.int32, (tall, LANES), 1) == ep_me * count + e
        for b in range(total // tall):
            rows, taken = pl.ds(b * tall, tall), pl.ds(b * many, many)
            slot = jnp.sum(jnp.where(at, slot_ref[rows, :], 0.0), axis=1, keepdims=True)
            seat = lax.broadcasted_iota(jnp.int32, (tall, many), 1) + b * many
            pick = (seat.astype(F32) == slot).astype(BF16)
            units = jnp.concatenate([ref[n, taken, :] for ref in hid_refs], axis=1)
            spread = jnp.dot(pick, units, preferred_element_type=F32).astype(BF16)
            for i in range(pieces):
                to = pl.multiple_of(n * full + place[i] * part, part)
                all_ref[rows, pl.ds(to, part)] = spread[:, i * part : (i + 1) * part]
    size = max(1, len(experts) // 2)
    for first in range(0, len(experts), size):
        if first < len(held):
            weights = now_ref[0]
        else:
            at = first - len(held)
            for e in streamed[at : at + size]:
                copies[e][0].wait()
            weights = late_ref[0, pl.ds(at, size)]
        weights = weights.reshape(size * full, weights.shape[-1])
        for b in range(total // tall):
            rows = pl.ds(b * tall, tall)
            product = jnp.dot(
                all_ref[rows, pl.ds(first * full, size * full)],
                weights,
                preferred_element_type=F32,
            )
            if first:
                product = acc_ref[rows, :] + product
            elif before_ref is not None:
                product = before_ref[rows, :] + product
            acc_ref[rows, :] = product
    if ahead:
        for e in ahead:
            more[e][0].wait()
    elif few:
        tokens = total // n_ep
        for s, out in enumerate(outs):
            rows = pl.ds(pl.multiple_of(owner[s] * tokens, tokens), tokens)
            out[...] = acc_ref[rows, :].astype(BF16)
    else:
        outs[0][...] = acc_ref[...].astype(BF16)


def place_kernel(n_tp, n_dp, *refs):
    pieces, out_ref, sems = refs[:-2], refs[-2], refs[-1]
    feat = pieces[0].shape[1]
    copies = [
        pltpu.make_async_copy(
            ref, out_ref.at[:, pl.ds(pl.multiple_of(to * feat, LANES), feat)], sems.at[i]
        )
        for i, (ref, to) in enumerate(zip(pieces, places(n_tp, n_dp)))
    ]
    for c in copies:
        c.start()
    for c in copies:
        c.wait()


def per_device(tokens, route_weights, expert_ids, gate_weight, up_weight, down_weight):
    n_ep, n_tp, n_dp = (lax.axis_size(a) for a in ("ep", "tp", "dp"))
    tok, width = tokens.shape
    top = expert_ids.shape[1]
    exp_local, _, part = gate_weight.shape
    feat = down_weight.shape[2]
    pieces = n_tp * n_dp
    devices = n_ep * pieces
    total = devices * tok
    slots = devices * CAP
    few = n_ep <= FEW

    def spread(x):
        out = []
        for a in range(n_tp):
            piece = meet(x, "tp", a) if a else x
            out += [meet(piece, "dp", b) if b else piece for b in range(n_dp)]
        return out

    packed = call(
        pack_kernel,
        [HBM] * 3,
        [((tok, width + LANES), BF16)],
        (hbm(tokens), hbm(route_weights), hbm(expert_ids)),
        [
            pltpu.VMEM((tok, top), F32),
            pltpu.VMEM((tok, top), jnp.int32),
            pltpu.SemaphoreType.DMA((3,)),
        ],
        limit=1,
    )[0]
    weights = [gate_weight, up_weight]
    full = part * pieces
    groups = 2 if exp_local % 2 == 0 else 1
    each = exp_local // groups
    ahead = [3 * exp_local // 8, exp_local // 4][:groups]
    held = [list(range(sum(ahead[:g]), sum(ahead[: g + 1]))) for g in range(groups)]
    others = list(range(sum(ahead), exp_local))
    streamed = []
    for g in range(groups):
        n = each - ahead[g]
        streamed.append(others[:n])
        others = others[n:]
    fetched, arrays = [], []
    if few:
        order = [0] + steps_of(n_ep)
        got = {s: meet(packed, "ep", s) for s in order if s}
        got[0] = packed
        chunks = [order[: (n_ep + 1) // 2], order[(n_ep + 1) // 2 :]]
        chunks = [c for c in chunks if c]
    else:
        chunks = [n_ep]
    for c, owner in enumerate(chunks):
        if few:
            rows = call(
                join_kernel,
                [VMEM] * len(owner),
                [((len(owner) * tok, width + LANES), BF16)],
                [vmem(got[s]) for s in owner],
                limit=1,
            )[0]
        else:
            rows = lax.all_gather(packed, "ep", axis=0, tiled=True)
        if c < groups and ahead[c]:
            fetched.append(fetch(weights, held[c][0], ahead[c], rows))
        arrays += spread(rows)
    blocks = (max(1, total // ROWS), LANES, min(total, ROWS))
    unit = ((each, slots, part), BF16)
    dma = lambda *n: pltpu.SemaphoreType.DMA(n)

    def late(g):
        n = len(streamed[g])
        return [pltpu.VMEM((2, n, width, part), BF16), dma(2, n)]

    again = [((total, width + LANES), BF16), ((total, LANES), F32), (blocks, F32)]
    hidden, slot, *again = call(
        functools.partial(first_kernel, (n_tp, n_dp, top, tok), chunks, held[0], streamed[0]),
        [VMEM] * (len(arrays) + len(fetched[:1])) + [HBM] * 2,
        [unit, ((total, LANES), F32)] + (again if groups == 2 else []),
        (*map(vmem, arrays), *map(vmem, fetched[:1]), *map(hbm, weights)),
        ([] if groups == 2 else [pltpu.VMEM(*a) for a in again]) + late(0),
        limit=12 if few else 40,
    )
    units = [spread(hidden)]
    if groups == 2:
        hidden = call(
            functools.partial(second_kernel, tok, held[1], streamed[1]),
            [VMEM] * 4 + [HBM] * 2,
            [unit],
            (*map(vmem, [fetched[1], *again]), *map(hbm, weights)),
            late(1),
            limit=18,
            flops=int(6e8),
        )[0]
        units.append(spread(hidden))

    shapes = [(total // n_ep, feat)] * n_ep if few else [(total, feat)]
    down_weight = hbm(down_weight.reshape(exp_local, full, feat))
    sums = (total, feat)
    now = []
    for g in range(groups):
        last = g == groups - 1
        order = held[g] + streamed[g]
        kept = order[: each // 2] if g else []
        rest = order[len(kept) :]
        coming = [] if last else (held[g + 1] + streamed[g + 1])[: each // 2]
        out = call(
            functools.partial(down_kernel, n_ep, n_tp, n_dp, few, kept, rest, coming),
            [VMEM] * (pieces + 1) + [HBM] + [VMEM] * len(now),
            [(s, BF16) for s in shapes]
            if last
            else [(sums, F32), ((1, len(coming), full, feat), BF16)],
            (*map(vmem, [*units[g], slot]), down_weight, *map(vmem, now)),
            [
                pltpu.VMEM(sums, F32) if last else dma(1, len(coming)),
                pltpu.VMEM((1, len(rest), full, feat), BF16),
                dma(1, len(rest)),
                pltpu.VMEM((total, each * full), BF16),
            ],
            limit=18 if few else 36,
            flops=int(6e8),
        )
        if last:
            partial = out
        else:
            now = [out[1], out[0]]

    if few:
        mine = partial[0].astype(F32)
        back = {s: meet(partial[s], "ep", s) for s in steps_of(n_ep)}
        for s in range(1, n_ep):
            mine = mine + back[s].astype(F32)
    else:
        back = lax.all_to_all(partial[0], "ep", split_axis=0, concat_axis=0, tiled=True)
        mine = jnp.sum(back.reshape(n_ep, total // n_ep, feat).astype(F32), axis=0)
    mine = mine.astype(BF16)

    around = places(n_tp, n_dp)
    final = []
    for i in range(pieces):
        a, b = i // n_dp, i % n_dp
        give = lax.dynamic_slice_in_dim(mine, around[i] * tok, tok, axis=0)
        if i:
            pairs = [
                (t * n_dp + d, (mate(t, a, n_tp) if a else t) * n_dp + (mate(d, b, n_dp) if b else d))
                for t in range(n_tp)
                for d in range(n_dp)
            ]
            give = lax.ppermute(give, ("tp", "dp"), pairs)
        final.append(give)
    return pl.pallas_call(
        functools.partial(place_kernel, n_tp, n_dp),
        in_specs=[VMEM] * pieces,
        out_specs=HBM,
        out_shape=jax.ShapeDtypeStruct((tok, pieces * feat), BF16),
        scratch_shapes=[pltpu.SemaphoreType.DMA((pieces,))],
        name="place",
        compiler_params=pltpu.CompilerParams(vmem_limit_bytes=1 << 20),
    )(*map(vmem, final))


def solution(mesh):
    spec = P(("groups", "ep", "tp", "dp"), None)
    weight = P("ep", None, ("tp", "dp"))

    return jax.shard_map(
        per_device,
        mesh=mesh,
        in_specs=(spec, spec, spec, weight, weight, weight),
        out_specs=spec,
        check_vma=False,
    )
```
